32 devices in a mesh: band: 4 (over y, x), ga: 8 (over z, core).
Axes of the slice: x: 2, y: 2, z: 4, core: 2. Of those that a mesh axis runs over, the one named last changes fastest.
Arguments:
- wavefunctions: bfloat16 [512, 98304], P('band', 'ga'), may hold values from -6 to 6
- projectors: bfloat16 [2048, 98304], P('band', 'ga'), may hold values from -0.125 to 0.125
- kinetic_diag: float32 [98304], P('ga'), may hold values from 0.1 to 4
- species_index: int32 [256], replicated, may hold values from 0 to 3
- coupling: float32 [4, 8, 8], replicated, may hold values from -5 to 5
Outputs:
- applied: bfloat16 [512, 98304], P('band', 'ga')
The draws below stay inside these ranges and needn't reach their ends.
All inputs are finite; a program needn't handle non-finite values.
Results may differ from the reference program's by a relative error of at most 0.015.
Values may be sent and summed in bfloat16 or wider, within the bound.
A program may use at most 64 MiB of HBM per device.

```python
import math
import jax
import jax.numpy as jnp
from jax import lax

NG = 98304
NPA = 8
ATOMS = 256
NSPEC = 4
BANDS = 512
NPROJ = 2048


def place_ends(array, rng, low, top_value):
    longest = array.shape.index(max(array.shape))
    spots = []
    for shift in (0, 1):
        where = [jax.random.randint(jax.random.fold_in(rng, axis), (), 0, length) for axis, length in enumerate(array.shape)]
        where[longest] = (where[longest] + shift) % array.shape[longest]
        spots.append(tuple(where))
    return array.at[spots[0]].set(low).at[spots[1]].set(top_value)


def shard_levels(rng, extent, split, smallest, largest):
    def one(axis_at, shards_of):
        steps = jax.random.uniform(jax.random.fold_in(jax.random.fold_in(rng, 6), axis_at), (shards_of,), jnp.float32, smallest / len(split), largest / len(split))
        return jnp.repeat(jnp.exp(steps), extent[axis_at] // shards_of).reshape((-1,) + (1,) * (len(extent) - axis_at - 1))

    gain = one(*split[0])
    for cut in split[1:]:
        gain = gain * one(*cut)
    return gain


def noise(rng, dims, spread, reach, shards=(), held_as=jnp.bfloat16):
    values = spread * jax.random.normal(rng, dims, jnp.float32)
    if shards:
        values = values * shard_levels(rng, dims, shards, -0.22, 0.18)
    return jnp.clip(values, -reach, reach).astype(held_as)


def setup_inputs(seed: int = 0) -> dict:
    splits = jax.random.split(jax.random.key(seed), 6)
    return {
        "wavefunctions": noise(splits[0], (BANDS, NG), 1.0, 6.0, ((0, 4), (1, 8))),
        "projectors": noise(splits[1], (NPROJ, NG), ((NG * NPROJ) ** -0.25), 0.125, ((0, 4), (1, 8))),
        "kinetic_diag": jnp.clip(jnp.exp(math.log(4.0) - 3.6888794 * jax.random.uniform(splits[2], (NG,), jnp.float32) ** shard_levels(splits[2], (NG,), ((0, 8),), -0.2, 0.2)), 0.1, 4.0),
        "species_index": place_ends(jax.random.randint(splits[3], (ATOMS,), 0, NSPEC), jax.random.fold_in(splits[3], 1), 0, NSPEC - 1).astype(jnp.int32),
        "coupling": noise(splits[4], (NSPEC, NPA, NPA), 0.35, 5.0, (), jnp.float32),
    }


def reference(wavefunctions, projectors, kinetic_diag, species_index, coupling):
    correlations = jnp.dot(wavefunctions, projectors.T, preferred_element_type=jnp.float32)
    onehot = (species_index[:, None] == jnp.arange(NSPEC, dtype=jnp.int32)[None, :]).astype(jnp.float32)
    blocks = jnp.einsum("as,sij->aij", onehot, coupling, precision=lax.Precision.HIGHEST)
    mixed = jnp.einsum("baj,aij->bai", correlations.reshape(BANDS, ATOMS, NPA), blocks, precision=lax.Precision.HIGHEST)
    mixed = mixed.reshape(BANDS, NPROJ).astype(jnp.bfloat16)
    nonlocal_term = jnp.dot(mixed, projectors, preferred_element_type=jnp.float32)
    return (kinetic_diag[None, :] * wavefunctions.astype(jnp.float32) + nonlocal_term).astype(jnp.bfloat16)
```

```python
import functools

import jax
import jax.numpy as jnp
from jax import lax
from jax.experimental import pallas as pl
from jax.experimental.pallas import tpu as pltpu
from jax.sharding import PartitionSpec as P

CHUNKS = 2
TILES = 4
LANES = 128

NPA = 8


def apply_blocks(correlations, species_index, coupling, atom_start):
    rows = correlations.shape[0]
    count = correlations.shape[1] // NPA
    local_species = lax.dynamic_slice_in_dim(species_index, atom_start, count)
    onehot = (
        local_species[:, None] == jnp.arange(coupling.shape[0], dtype=jnp.int32)[None, :]
    ).astype(jnp.float32)
    blocks = jnp.einsum("as,sij->aij", onehot, coupling, precision=lax.Precision.HIGHEST)
    mixed = jnp.einsum(
        "baj,aij->bai",
        correlations.reshape(rows, count, NPA),
        blocks,
        precision=lax.Precision.HIGHEST,
    )
    return mixed.reshape(rows, count * NPA).astype(jnp.bfloat16)


def reduce_and_mix(partial_value, species_index, coupling, first_proj):
    total = lax.psum(partial_value.astype(jnp.bfloat16), "ga").astype(jnp.float32)
    return apply_blocks(total, species_index, coupling, first_proj // NPA)


def local(wavefunctions, projectors, kinetic_diag, species_index, coupling):
    proj_local = projectors.shape[0]
    band_index = lax.axis_index("band")
    partial_value = jnp.einsum(
        "bg,pg->bp",
        lax.all_gather(wavefunctions, "band", axis=0, tiled=True),
        projectors,
        preferred_element_type=jnp.float32,
    )
    mixed = reduce_and_mix(partial_value, species_index, coupling, band_index * proj_local)
    nonlocal_term = lax.psum_scatter(
        jnp.dot(mixed, projectors, preferred_element_type=jnp.float32).astype(jnp.bfloat16),
        "band",
        scatter_dimension=0,
        tiled=True,
    ).astype(jnp.float32)
    return (kinetic_diag[None, :] * wavefunctions.astype(jnp.float32) + nonlocal_term).astype(
        jnp.bfloat16
    )


def mixing_tiles(species_index, coupling, first_atom, count):
    npa = coupling.shape[1]
    local_species = lax.dynamic_slice_in_dim(species_index, first_atom, count)
    onehot = (
        local_species[:, None] == jnp.arange(coupling.shape[0], dtype=jnp.int32)[None, :]
    ).astype(jnp.float32)
    per_tile = LANES // npa
    spread = jnp.einsum("as,sij->jai", onehot, coupling, precision=lax.Precision.HIGHEST)
    spread = spread.reshape(npa, count // per_tile, LANES).transpose(1, 0, 2)
    spread = jnp.tile(spread, (1, per_tile, 1))
    atom_of = jnp.arange(LANES) // npa
    return jnp.where(atom_of[:, None] == atom_of[None, :], spread, 0.0)


def kernel(
    nga, wf, pj, tiles, out,
    proj, wave, acc, csend, crecv, sumf, sumb, parts, mine, theirs, nsend, nrecv, nkeep, nfull,
    s_loc, s_p, s_wm, s_wo, s_wf, s_a, s_c, s_d, s_f, s_n, s_o,
):
    chunks, _, rows, half = wave.shape
    width = nsend.shape[-1]
    quarter = nga // 4
    band, me = lax.axis_index("band"), lax.axis_index("ga")
    core, y, x = me % 2, band // 2, band % 2
    across_x, across_y, diag = y * 2 + 1 - x, (1 - y) * 2 + x, 3 - band
    m = (1 - core) * y + core * x
    m_nbr = (1 - core) * across_y + core * across_x
    o_nbr = (1 - core) * across_x + core * across_y
    here = pl.multiple_of(m * half, LANES)
    there = pl.multiple_of((1 - m) * half, LANES)
    to_m, to_o = {"band": m_nbr}, {"band": o_nbr}

    def remote(src, dst, sems, device):
        return pltpu.make_async_remote_copy(
            src_ref=src, dst_ref=dst, send_sem=sems.at[0], recv_sem=sems.at[1],
            device_id=device, device_id_type=pl.DeviceIdType.MESH,
        )

    def span(k):
        return pl.ds(k * rows, rows)

    local_p = pltpu.make_async_copy(pj.at[:, pl.ds(here, half)], proj.at[0], s_loc.at[0])
    local_w = [
        pltpu.make_async_copy(wf.at[span(k), pl.ds(here, half)], wave.at[k, band], s_loc.at[1 + k])
        for k in range(chunks)
    ]
    send_p = remote(pj.at[:, pl.ds(there, half)], proj.at[1], s_p, to_m)
    send_wm = [
        remote(wf.at[span(k), pl.ds(there, half)], wave.at[k, band], s_wm.at[k], to_m)
        for k in range(chunks)
    ]
    send_wo = [
        remote(wf.at[span(k), pl.ds(here, half)], wave.at[k, band], s_wo.at[k], to_o)
        for k in range(chunks)
    ]
    send_wf = [
        remote(wave.at[k, m_nbr], wave.at[k, m_nbr], s_wf.at[k], to_o) for k in range(chunks)
    ]
    send_a = [remote(csend.at[k], crecv.at[k], s_a.at[k], to_m) for k in range(chunks)]
    send_f = [remote(mine.at[k], theirs.at[k], s_f.at[k], to_m) for k in range(chunks)]

    def peer(step):
        return (me + step + 1) % nga

    def send_c(k, step):
        return remote(
            sumb.at[k, peer(step)], parts.at[k, step], s_c.at[k, step], {"ga": peer(step)}
        )

    def send_d(k, step):
        return remote(mine.at[k, me], mine.at[k, me], s_d.at[k, step], {"ga": peer(step)})

    def send_n(k, t):
        return remote(nsend.at[k, t], nrecv.at[k, t], s_n.at[k, t], to_o)

    def send_o(k, t):
        place = out.at[span(k), pl.ds(pl.multiple_of(here + t * width, LANES), width)]
        return remote(nfull.at[k, t], place, s_o.at[k, t], to_m)

    def each_peer(body):
        def step(i, carry):
            body(i)
            return carry

        lax.fori_loop(0, nga - 1, step, 0)

    def each_tile(body, first=0, last=TILES):
        def step(i, carry):
            body(i)
            return carry

        lax.fori_loop(first, last, step, 0)

    def correlate(k, slot):
        acc[...] = jnp.zeros_like(acc)

        def tile(t):
            cols = pl.ds(pl.multiple_of(t * width, LANES), width)
            acc[...] += lax.dot_general(
                wave[k, :, :, cols].reshape(4 * rows, width),
                proj[slot, :, cols],
                (((1,), (1,)), ((), ())),
                preferred_element_type=jnp.float32,
            )

        each_tile(tile)

    def first(k):
        local_w[k].wait()
        send_wo[k].wait_recv()
        send_wf[k].wait_recv()
        correlate(k, 1)
        csend[k] = acc[...].astype(jnp.bfloat16)
        send_a[k].start()
        correlate(k, 0)
        sumf[k] = acc[...].reshape(sumf.shape[1:])

    def reduce_start(k):
        send_a[k].wait_recv()
        total = sumf[k] + crecv[k].astype(jnp.float32).reshape(sumf.shape[1:])
        sumf[k] = total
        sumb[k] = total.astype(jnp.bfloat16)
        each_peer(lambda step: send_c(k, step).start())

    def mix_start(k):
        each_peer(lambda step: send_c(k, step).wait_recv())
        total = sumf[k, me]
        for step in range(nga - 1):
            total = total + parts[k, step].astype(jnp.float32)
        for t in range(tiles.shape[0]):
            cols = slice(t * LANES, (t + 1) * LANES)
            mine[k, me, :, cols] = jnp.dot(
                total[:, cols], tiles[t],
                preferred_element_type=jnp.float32, precision=lax.Precision.HIGHEST,
            ).astype(jnp.bfloat16)
        each_peer(lambda step: send_d(k, step).start())

    def share_start(k):
        each_peer(lambda step: send_d(k, step).wait_recv())
        send_f[k].start()

    def second(k):
        send_f[k].wait_recv()

        def ordered(ref):
            picks = [ref[k, pl.ds(b * quarter, quarter)] for b in (o_nbr, diag, band, m_nbr)]
            return jnp.concatenate(picks, axis=0).reshape(4 * rows, ref.shape[-1])

        def tile(t):
            cols = pl.ds(pl.multiple_of(t * width, LANES), width)
            value = jnp.dot(ordered(mine), proj[0, :, cols], preferred_element_type=jnp.float32)
            value += jnp.dot(ordered(theirs), proj[1, :, cols], preferred_element_type=jnp.float32)
            value = value.reshape(4, rows, width)
            nsend[k, t] = value[:2].astype(jnp.bfloat16)
            send_n(k, t).start()
            nkeep[k, t] = value[2:]

        each_tile(tile)

    def finish(k, begin, end):
        def tile(t):
            send_n(k, t).wait_recv()
            nfull[k, t] = (nkeep[k, t, 1] + nrecv[k, t, 1].astype(jnp.float32)).astype(jnp.bfloat16)
            send_o(k, t).start()
            cols = pl.ds(pl.multiple_of(here + t * width, LANES), width)
            out[span(k), cols] = (nkeep[k, t, 0] + nrecv[k, t, 0].astype(jnp.float32)).astype(
                jnp.bfloat16
            )

        each_tile(tile, begin, end)

    local_p.start()
    for k in range(chunks):
        local_w[k].start()
    barrier = pltpu.get_barrier_semaphore()
    for device in (to_m, to_o):
        pl.semaphore_signal(
            barrier, inc=1, device_id=device, device_id_type=pl.DeviceIdType.MESH
        )
    each_peer(
        lambda step: pl.semaphore_signal(
            barrier, inc=1, device_id={"ga": peer(step)}, device_id_type=pl.DeviceIdType.MESH
        )
    )
    pl.semaphore_wait(barrier, nga + 1)

    send_wm[0].start()
    send_wo[0].start()
    send_p.start()
    for k in range(1, chunks):
        send_wm[k].start()
    send_wm[0].wait_recv()
    send_wf[0].start()
    local_p.wait()
    send_p.wait_recv()
    for k in range(1, chunks):
        send_wo[k].start()

    first(0)
    reduce_start(0)
    for k in range(1, chunks):
        send_wm[k].wait_recv()
        send_wf[k].start()
    mix_start(0)
    for k in range(1, chunks):
        first(k)
        share_start(k - 1)
        reduce_start(k)
        second(k - 1)
        mix_start(k)
        finish(k - 1, 0, TILES // 2)
        if k == chunks - 1:
            share_start(k)
        finish(k - 1, TILES // 2, TILES)
    if chunks == 1:
        share_start(0)
    second(chunks - 1)
    finish(chunks - 1, 0, TILES)

    send_p.wait_send()
    for k in range(chunks):
        for copy in (send_wm[k], send_wo[k], send_wf[k], send_a[k], send_f[k]):
            copy.wait_send()
        each_peer(lambda step: send_c(k, step).wait_send())
        each_peer(lambda step: send_d(k, step).wait_send())
        each_tile(lambda t: send_n(k, t).wait_send())
        each_tile(lambda t: send_o(k, t).wait())


def square(nga, wavefunctions, projectors, kinetic_diag, species_index, coupling):
    bands, waves = wavefunctions.shape
    count = projectors.shape[0]
    npa = coupling.shape[1]
    half, rows = waves // 2, bands // CHUNKS
    width, share = half // TILES, 4 * rows // nga
    tiles = mixing_tiles(
        species_index, coupling, lax.axis_index("band") * (count // npa), count // npa
    )
    bf16, f32 = jnp.bfloat16, jnp.float32
    dma = pltpu.SemaphoreType.DMA
    nonlocal_term = pl.pallas_call(
        functools.partial(kernel, nga),
        out_shape=jax.ShapeDtypeStruct((bands, waves), bf16),
        in_specs=[
            pl.BlockSpec(memory_space=pl.ANY),
            pl.BlockSpec(memory_space=pl.ANY),
            pl.BlockSpec(memory_space=pltpu.VMEM),
        ],
        out_specs=pl.BlockSpec(memory_space=pltpu.VMEM),
        scratch_shapes=[
            pltpu.VMEM((2, count, half), bf16),
            pltpu.VMEM((CHUNKS, 4, rows, half), bf16),
            pltpu.VMEM((4 * rows, count), f32),
            pltpu.VMEM((CHUNKS, 4 * rows, count), bf16),
            pltpu.VMEM((CHUNKS, 4 * rows, count), bf16),
            pltpu.VMEM((CHUNKS, nga, share, count), f32),
            pltpu.VMEM((CHUNKS, nga, share, count), bf16),
            pltpu.VMEM((CHUNKS, nga - 1, share, count), bf16),
            pltpu.VMEM((CHUNKS, nga, share, count), bf16),
            pltpu.VMEM((CHUNKS, nga, share, count), bf16),
            pltpu.VMEM((CHUNKS, TILES, 2, rows, width), bf16),
            pltpu.VMEM((CHUNKS, TILES, 2, rows, width), bf16),
            pltpu.VMEM((CHUNKS, TILES, 2, rows, width), f32),
            pltpu.VMEM((CHUNKS, TILES, rows, width), bf16),
            dma((1 + CHUNKS,)),
            dma((2,)),
            dma((CHUNKS, 2)),
            dma((CHUNKS, 2)),
            dma((CHUNKS, 2)),
            dma((CHUNKS, 2)),
            dma((CHUNKS, nga - 1, 2)),
            dma((CHUNKS, nga - 1, 2)),
            dma((CHUNKS, 2)),
            dma((CHUNKS, TILES, 2)),
            dma((CHUNKS, TILES, 2)),
        ],
        compiler_params=pltpu.CompilerParams(
            collective_id=0, has_side_effects=True, vmem_limit_bytes=60 * 2**20
        ),
    )(wavefunctions, projectors, tiles)
    return (
        kinetic_diag[None, :] * wavefunctions.astype(f32) + nonlocal_term.astype(f32)
    ).astype(bf16)


def solution(mesh):
    in_specs = (P("band", "ga"), P("band", "ga"), P("ga"), P(), P())
    out_specs = P("band", "ga")
    nga = mesh.shape["ga"]
    fits = mesh.shape["band"] == 4 and nga % 4 == 0
    body = functools.partial(square, nga) if fits else local
    return jax.shard_map(body, mesh=mesh, in_specs=in_specs, out_specs=out_specs, check_vma=False)
```

```python
import functools

import jax
import jax.numpy as jnp
from jax import lax
from jax.experimental import pallas as pl
from jax.experimental.pallas import tpu as pltpu
from jax.sharding import PartitionSpec as P

CHUNKS = 2
TILES = 4
LANES = 128

NPA = 8


def apply_blocks(correlations, species_index, coupling, atom_start):
    rows = correlations.shape[0]
    count = correlations.shape[1] // NPA
    local_species = lax.dynamic_slice_in_dim(species_index, atom_start, count)
    onehot = (
        local_species[:, None] == jnp.arange(coupling.shape[0], dtype=jnp.int32)[None, :]
    ).astype(jnp.float32)
    blocks = jnp.einsum("as,sij->aij", onehot, coupling, precision=lax.Precision.HIGHEST)
    mixed = jnp.einsum(
        "baj,aij->bai",
        correlations.reshape(rows, count, NPA),
        blocks,
        precision=lax.Precision.HIGHEST,
    )
    return mixed.reshape(rows, count * NPA).astype(jnp.bfloat16)


def reduce_and_mix(partial_value, species_index, coupling, first_proj):
    total = lax.psum(partial_value.astype(jnp.bfloat16), "ga").astype(jnp.float32)
    return apply_blocks(total, species_index, coupling, first_proj // NPA)


def local(wavefunctions, projectors, kinetic_diag, species_index, coupling):
    proj_local = projectors.shape[0]
    band_index = lax.axis_index("band")
    partial_value = jnp.einsum(
        "bg,pg->bp",
        lax.all_gather(wavefunctions, "band", axis=0, tiled=True),
        projectors,
        preferred_element_type=jnp.float32,
    )
    mixed = reduce_and_mix(partial_value, species_index, coupling, band_index * proj_local)
    nonlocal_term = lax.psum_scatter(
        jnp.dot(mixed, projectors, preferred_element_type=jnp.float32).astype(jnp.bfloat16),
        "band",
        scatter_dimension=0,
        tiled=True,
    ).astype(jnp.float32)
    return (kinetic_diag[None, :] * wavefunctions.astype(jnp.float32) + nonlocal_term).astype(
        jnp.bfloat16
    )


def mixing_tiles(species_index, coupling, first_atom, count):
    npa = coupling.shape[1]
    local_species = lax.dynamic_slice_in_dim(species_index, first_atom, count)
    onehot = (
        local_species[:, None] == jnp.arange(coupling.shape[0], dtype=jnp.int32)[None, :]
    ).astype(jnp.float32)
    per_tile = LANES // npa
    spread = jnp.einsum("as,sij->jai", onehot, coupling, precision=lax.Precision.HIGHEST)
    spread = spread.reshape(npa, count // per_tile, LANES).transpose(1, 0, 2)
    spread = jnp.tile(spread, (1, per_tile, 1))
    atom_of = jnp.arange(LANES) // npa
    return jnp.where(atom_of[:, None] == atom_of[None, :], spread, 0.0)


def kernel(
    nga, wf, pj, tiles, out,
    proj, wave, acc, csend, crecv, sumf, sumb, parts, mine, theirs, nsend, nrecv, nfull,
    s_loc, s_p, s_wm, s_wo, s_wf, s_a, s_c, s_d, s_f, s_n, s_o,
):
    chunks, _, rows, half = wave.shape
    width = nsend.shape[-1]
    quarter = nga // 4
    band, me = lax.axis_index("band"), lax.axis_index("ga")
    core, y, x = me % 2, band // 2, band % 2
    across_x, across_y, diag = y * 2 + 1 - x, (1 - y) * 2 + x, 3 - band
    m = (1 - core) * y + core * x
    m_nbr = (1 - core) * across_y + core * across_x
    o_nbr = (1 - core) * across_x + core * across_y
    here = pl.multiple_of(m * half, LANES)
    there = pl.multiple_of((1 - m) * half, LANES)
    to_m, to_o = {"band": m_nbr}, {"band": o_nbr}

    def remote(src, dst, sems, device):
        return pltpu.make_async_remote_copy(
            src_ref=src, dst_ref=dst, send_sem=sems.at[0], recv_sem=sems.at[1],
            device_id=device, device_id_type=pl.DeviceIdType.MESH,
        )

    def span(k):
        return pl.ds(k * rows, rows)

    local_p = pltpu.make_async_copy(pj.at[:, pl.ds(here, half)], proj.at[0], s_loc.at[0])
    local_w = [
        pltpu.make_async_copy(wf.at[span(k), pl.ds(here, half)], wave.at[k, band], s_loc.at[1 + k])
        for k in range(chunks)
    ]
    send_p = remote(pj.at[:, pl.ds(there, half)], proj.at[1], s_p, to_m)
    send_wm = [
        remote(wf.at[span(k), pl.ds(there, half)], wave.at[k, band], s_wm.at[k], to_m)
        for k in range(chunks)
    ]
    send_wo = [
        remote(wf.at[span(k), pl.ds(here, half)], wave.at[k, band], s_wo.at[k], to_o)
        for k in range(chunks)
    ]
    send_wf = [
        remote(wave.at[k, m_nbr], wave.at[k, m_nbr], s_wf.at[k], to_o) for k in range(chunks)
    ]
    send_a = [remote(csend.at[k], crecv.at[k], s_a.at[k], to_m) for k in range(chunks)]
    send_f = [remote(mine.at[k], theirs.at[k], s_f.at[k], to_m) for k in range(chunks)]

    def peer(step):
        return (me + step + 1) % nga

    def send_c(k, step):
        return remote(
            sumb.at[k, peer(step)], parts.at[k, step], s_c.at[k, step], {"ga": peer(step)}
        )

    def send_d(k, step):
        return remote(mine.at[k, me], mine.at[k, me], s_d.at[k, step], {"ga": peer(step)})

    def send_n(k, t):
        return remote(nsend.at[k, t], nrecv.at[k, t], s_n.at[k, t], to_o)

    def send_o(k, t):
        place = out.at[span(k), pl.ds(pl.multiple_of(here + t * width, LANES), width)]
        return remote(nfull.at[k, t], place, s_o.at[k, t], to_m)

    def each_peer(body):
        def step(i, carry):
            body(i)
            return carry

        lax.fori_loop(0, nga - 1, step, 0)

    def each_tile(body, first=0, last=TILES):
        def step(i, carry):
            body(i)
            return carry

        lax.fori_loop(first, last, step, 0)

    def correlate(k, slot):
        acc[...] = jnp.zeros_like(acc)

        def tile(t):
            cols = pl.ds(pl.multiple_of(t * width, LANES), width)
            acc[...] += lax.dot_general(
                wave[k, :, :, cols].reshape(4 * rows, width),
                proj[slot, :, cols],
                (((1,), (1,)), ((), ())),
                preferred_element_type=jnp.float32,
            )

        each_tile(tile)

    def first(k):
        local_w[k].wait()
        send_wo[k].wait_recv()
        send_wf[k].wait_recv()
        if k == 0:
            correlate(k, 0)
            sumf[k] = acc[...].reshape(sumf.shape[1:])
            send_p.wait_recv()
        correlate(k, 1)
        csend[k] = acc[...].astype(jnp.bfloat16)
        send_a[k].start()
        if k > 0:
            correlate(k, 0)
            sumf[k] = acc[...].reshape(sumf.shape[1:])

    def reduce_start(k):
        send_a[k].wait_recv()
        total = sumf[k] + crecv[k].astype(jnp.float32).reshape(sumf.shape[1:])
        sumf[k] = total
        sumb[k] = total.astype(jnp.bfloat16)
        each_peer(lambda step: send_c(k, step).start())

    def mix_start(k):
        each_peer(lambda step: send_c(k, step).wait_recv())
        total = sumf[k, me]
        for step in range(nga - 1):
            total = total + parts[k, step].astype(jnp.float32)
        for t in range(tiles.shape[0]):
            cols = slice(t * LANES, (t + 1) * LANES)
            mine[k, me, :, cols] = jnp.dot(
                total[:, cols], tiles[t],
                preferred_element_type=jnp.float32, precision=lax.Precision.HIGHEST,
            ).astype(jnp.bfloat16)
        each_peer(lambda step: send_d(k, step).start())

    def share_start(k):
        each_peer(lambda step: send_d(k, step).wait_recv())
        send_f[k].start()

    def ordered(ref, k, blocks):
        picks = [ref[k, pl.ds(b * quarter, quarter)] for b in blocks]
        return jnp.concatenate(picks, axis=0).reshape(2 * rows, ref.shape[-1])

    def expand(k, t, blocks):
        cols = pl.ds(pl.multiple_of(t * width, LANES), width)
        value = jnp.dot(
            ordered(mine, k, blocks), proj[0, :, cols], preferred_element_type=jnp.float32
        )
        value += jnp.dot(
            ordered(theirs, k, blocks), proj[1, :, cols], preferred_element_type=jnp.float32
        )
        return value.reshape(2, rows, width)

    def second(k):
        send_f[k].wait_recv()

        def tile(t):
            nsend[k, t] = expand(k, t, (o_nbr, diag)).astype(jnp.bfloat16)
            send_n(k, t).start()

        each_tile(tile)

    def finish(k, begin, end):
        def tile(t):
            value = expand(k, t, (band, m_nbr))
            send_n(k, t).wait_recv()
            value += nrecv[k, t].astype(jnp.float32)
            nfull[k, t] = value[1].astype(jnp.bfloat16)
            send_o(k, t).start()
            cols = pl.ds(pl.multiple_of(here + t * width, LANES), width)
            out[span(k), cols] = value[0].astype(jnp.bfloat16)

        each_tile(tile, begin, end)

    local_p.start()
    for k in range(chunks):
        local_w[k].start()
    barrier = pltpu.get_barrier_semaphore()
    for device in (to_m, to_o):
        pl.semaphore_signal(
            barrier, inc=1, device_id=device, device_id_type=pl.DeviceIdType.MESH
        )
    each_peer(
        lambda step: pl.semaphore_signal(
            barrier, inc=1, device_id={"ga": peer(step)}, device_id_type=pl.DeviceIdType.MESH
        )
    )
    pl.semaphore_wait(barrier, nga + 1)

    send_wm[0].start()
    send_wo[0].start()
    send_p.start()
    for k in range(1, chunks):
        send_wm[k].start()
    send_wm[0].wait_recv()
    send_wf[0].start()
    for k in range(1, chunks):
        send_wo[k].start()
    local_p.wait()

    first(0)
    reduce_start(0)
    for k in range(1, chunks):
        send_wm[k].wait_recv()
        send_wf[k].start()
    mix_start(0)
    for k in range(1, chunks):
        share_start(k - 1)
        first(k)
        second(k - 1)
        reduce_start(k)
        mix_start(k)
        finish(k - 1, 0, TILES // 2)
        if k == chunks - 1:
            share_start(k)
        finish(k - 1, TILES // 2, TILES)
    if chunks == 1:
        share_start(0)
    second(chunks - 1)
    finish(chunks - 1, 0, TILES)

    send_p.wait_send()
    for k in range(chunks):
        for copy in (send_wm[k], send_wo[k], send_wf[k], send_a[k], send_f[k]):
            copy.wait_send()
        each_peer(lambda step: send_c(k, step).wait_send())
        each_peer(lambda step: send_d(k, step).wait_send())
        each_tile(lambda t: send_n(k, t).wait_send())
        each_tile(lambda t: send_o(k, t).wait())


def square(nga, wavefunctions, projectors, kinetic_diag, species_index, coupling):
    bands, waves = wavefunctions.shape
    count = projectors.shape[0]
    npa = coupling.shape[1]
    half, rows = waves // 2, bands // CHUNKS
    width, share = half // TILES, 4 * rows // nga
    tiles = mixing_tiles(
        species_index, coupling, lax.axis_index("band") * (count // npa), count // npa
    )
    bf16, f32 = jnp.bfloat16, jnp.float32
    dma = pltpu.SemaphoreType.DMA
    nonlocal_term = pl.pallas_call(
        functools.partial(kernel, nga),
        out_shape=jax.ShapeDtypeStruct((bands, waves), bf16),
        in_specs=[
            pl.BlockSpec(memory_space=pl.ANY),
            pl.BlockSpec(memory_space=pl.ANY),
            pl.BlockSpec(memory_space=pltpu.VMEM),
        ],
        out_specs=pl.BlockSpec(memory_space=pltpu.VMEM),
        scratch_shapes=[
            pltpu.VMEM((2, count, half), bf16),
            pltpu.VMEM((CHUNKS, 4, rows, half), bf16),
            pltpu.VMEM((4 * rows, count), f32),
            pltpu.VMEM((CHUNKS, 4 * rows, count), bf16),
            pltpu.VMEM((CHUNKS, 4 * rows, count), bf16),
            pltpu.VMEM((CHUNKS, nga, share, count), f32),
            pltpu.VMEM((CHUNKS, nga, share, count), bf16),
            pltpu.VMEM((CHUNKS, nga - 1, share, count), bf16),
            pltpu.VMEM((CHUNKS, nga, share, count), bf16),
            pltpu.VMEM((CHUNKS, nga, share, count), bf16),
            pltpu.VMEM((CHUNKS, TILES, 2, rows, width), bf16),
            pltpu.VMEM((CHUNKS, TILES, 2, rows, width), bf16),
            pltpu.VMEM((CHUNKS, TILES, rows, width), bf16),
            dma((1 + CHUNKS,)),
            dma((2,)),
            dma((CHUNKS, 2)),
            dma((CHUNKS, 2)),
            dma((CHUNKS, 2)),
            dma((CHUNKS, 2)),
            dma((CHUNKS, nga - 1, 2)),
            dma((CHUNKS, nga - 1, 2)),
            dma((CHUNKS, 2)),
            dma((CHUNKS, TILES, 2)),
            dma((CHUNKS, TILES, 2)),
        ],
        compiler_params=pltpu.CompilerParams(
            collective_id=0, has_side_effects=True, vmem_limit_bytes=60 * 2**20
        ),
    )(wavefunctions, projectors, tiles)
    return (
        kinetic_diag[None, :] * wavefunctions.astype(f32) + nonlocal_term.astype(f32)
    ).astype(bf16)


def solution(mesh):
    in_specs = (P("band", "ga"), P("band", "ga"), P("ga"), P(), P())
    out_specs = P("band", "ga")
    nga = mesh.shape["ga"]
    fits = mesh.shape["band"] == 4 and nga % 4 == 0
    body = functools.partial(square, nga) if fits else local
    return jax.shard_map(body, mesh=mesh, in_specs=in_specs, out_specs=out_specs, check_vma=False)
```
